32 devices in a mesh: grid: 8 (over z, y), band: 4 (over x, core).
Axes of the slice: x: 2, y: 2, z: 4, core: 2. Of those that a mesh axis runs over, the one named last changes fastest.
Arguments:
- orbitals: float32 [32, 16, 16, 512], P('grid', None, None, 'band'), may hold values from -80 to 80
- projectors: float32 [32, 16, 16, 512], P('grid', None, None, 'band'), may hold values from -0.09375 to 0.09375
- potential: float32 [32, 16, 16], P('grid'), may hold values from 0.3 to 3
Outputs:
- updated_orbitals: float32 [32, 16, 16, 512], P('grid', None, None, 'band')
- rayleigh_quotients: float32 [3, 512], P(None, 'band')
- residual_norms: float32 [3, 512], P(None, 'band')
The draws below stay inside these ranges and needn't reach their ends.
All inputs are finite; a program needn't handle non-finite values.
Results may differ from the reference program's by a relative error of at most 0.00012.
Values sent between devices are 32-bit elements; how exact they have to be, the bound alone decides.
A program may use at most 128 MiB of HBM per device.

```python
import math
import jax
import jax.numpy as jnp
from jax import lax

NX = 16
NY = 16
BANDS = 512
NXI = 512
ITERS = 3
NZ = 32


def draw_orbitals(key, part):
    jitter_key = jax.random.fold_in(key, 11)
    scale_key = jax.random.fold_in(key, 12)
    height = jnp.arange(NZ, dtype=jnp.float32) / max(NZ - 1, 1)
    scales = jnp.exp(jax.random.uniform(scale_key, (BANDS,), jnp.float32, 0.0, math.log(10.0)))
    profile = 0.6 + 1.2 * height
    jitter = jnp.clip(jax.random.normal(jitter_key, (NZ, NX, NY, BANDS), jnp.float32), -4.0, 4.0)
    values = jitter * profile[:, None, None, None] * scales
    return values.astype(jnp.float32)


def steps_of(key, extent, shards, smallest, top_value):
    def one(axis_at, shards_of):
        draws = jax.random.uniform(jax.random.fold_in(jax.random.fold_in(key, 6), axis_at), (shards_of,), jnp.float32, smallest / len(shards), top_value / len(shards))
        return jnp.repeat(jnp.exp(draws), extent[axis_at] // shards_of).reshape((-1,) + (1,) * (len(extent) - axis_at - 1))

    gain = one(*shards[0])
    for cut in shards[1:]:
        gain = gain * one(*cut)
    return gain


def scatter_about(key, shape, spread, bound, split=(), held_as=jnp.bfloat16):
    factor_of = steps_of(key, shape, split, -0.22, 0.18) if split else 1.0
    values = jax.random.normal(key, shape, jnp.float32) * spread * factor_of
    return jnp.minimum(jnp.maximum(values, -bound), bound).astype(held_as)


def setup_inputs(seed: int = 0) -> dict:
    splits = jax.random.split(jax.random.key(seed), 4)
    return {
        "orbitals": draw_orbitals(jax.random.fold_in(splits[3], 71), 0),
        "projectors": scatter_about(splits[1], (NZ, NX, NY, NXI), ((2.0 / (NZ * NX * NY)) ** 0.5), 0.09375, ((0, 8), (3, 4)), jnp.float32),
        "potential": jnp.clip(jnp.exp(math.log(3.0) - 2.3025851 * jax.random.uniform(splits[2], (NZ, NX, NY), jnp.float32) ** steps_of(splits[2], (NZ, NX, NY), ((0, 8),), -0.2, 0.2)), 0.3, 3.0),
    }


STENCIL = (-205.0 / 72.0, 8.0 / 5.0, -1.0 / 5.0, 8.0 / 315.0, -1.0 / 560.0)
STEP_LENGTH = 0.25
NORM_EPS = 1e-06
HIGHEST = lax.Precision.HIGHEST

def laplacian(grid_field):
    result = 3.0 * STENCIL[0] * grid_field
    for dimension in (0, 1, 2):
        for distance in range(1, 5):
            result = result + STENCIL[distance] * (jnp.roll(grid_field, distance, dimension) + jnp.roll(grid_field, -distance, dimension))
    return result

def matmul(left, right):
    return jnp.dot(left.astype(jnp.float32), right.astype(jnp.float32), precision=HIGHEST, preferred_element_type=jnp.float32)

def reference(orbitals, projectors, potential):
    grid_shape = orbitals.shape
    vectors = orbitals.reshape(-1, BANDS)
    projector_rows = projectors.reshape(-1, NXI)
    identity_matrix = jnp.eye(BANDS, dtype=jnp.float32)
    quotient_list = []
    norm_list = []
    for iteration in range(ITERS):
        margin = matmul(vectors.T, vectors)
        factor = jnp.linalg.cholesky(margin)
        inverse = jax.scipy.linalg.solve_triangular(factor, identity_matrix, lower=True)
        vectors = matmul(vectors, inverse.T)
        coupling = matmul(projector_rows.T, vectors)
        exchange_part = matmul(projector_rows, coupling)
        grid_field = vectors.reshape(grid_shape)
        applied = (-0.5 * laplacian(grid_field) + potential[..., None] * grid_field).reshape(-1, BANDS) - exchange_part
        rayleigh = lax.optimization_barrier(jnp.sum(vectors * applied, axis=0))
        residual = applied - rayleigh[None, :] * vectors
        squared = lax.optimization_barrier(jnp.sum(residual * residual, axis=0))
        vectors = vectors - STEP_LENGTH * residual / jnp.sqrt(squared + NORM_EPS)[None, :]
        quotient_list.append(rayleigh)
        norm_list.append(jnp.sqrt(squared))
    return (vectors.reshape(grid_shape), jnp.stack(quotient_list), jnp.stack(norm_list))
```

```python
import functools

import jax
import jax.numpy as jnp
from jax import lax
from jax.experimental import pallas as pl
from jax.experimental.pallas import tpu as pltpu
from jax.sharding import PartitionSpec as P

ITERS = 3


STENCIL = (-205.0 / 72.0, 8.0 / 5.0, -1.0 / 5.0, 8.0 / 315.0, -1.0 / 560.0)
STEP_LENGTH = 0.25
NORM_EPS = 1e-06
HIGHEST = lax.Precision.HIGHEST
MESH = pl.DeviceIdType.MESH
VMEM = pl.BlockSpec(memory_space=pltpu.VMEM)


def with_halo(block, sides, width):
    for axis, dim in sides:
        count = lax.axis_size(axis)
        forward = [(i, i + 1) for i in range(count - 1)]
        forward.append((count - 1, 0))
        backward = [(target, source) for source, target in forward]
        low = lax.ppermute(
            lax.slice_in_dim(block, block.shape[dim] - width, None, axis=dim), axis, forward
        )
        high = lax.ppermute(lax.slice_in_dim(block, 0, width, axis=dim), axis, backward)
        block = jnp.concatenate([low, block, high], axis=dim)
    return block


def matmul(left, right):
    return jnp.dot(left, right, precision=HIGHEST, preferred_element_type=jnp.float32)


def laplacian(grid_field):
    padded = with_halo(grid_field, (("grid", 0),), 4)
    planes_here = grid_field.shape[0]
    result = 3.0 * STENCIL[0] * grid_field
    for distance in range(1, 5):
        result = result + STENCIL[distance] * (
            padded[4 + distance : 4 + distance + planes_here]
            + padded[4 - distance : 4 - distance + planes_here]
        )
    for dimension in (1, 2):
        for distance in range(1, 5):
            result = result + STENCIL[distance] * (
                jnp.roll(grid_field, distance, dimension)
                + jnp.roll(grid_field, -distance, dimension)
            )
    return result


def dot_in_kernel(left, right, contract):
    return lax.dot_general(
        left, right, (contract, ((), ())), precision=HIGHEST, preferred_element_type=jnp.float32
    )


def block_inverse_factor(block):
    size = block.shape[0]
    groups = [block[8 * g : 8 * g + 8, :] for g in range(size // 8)]
    lane = lax.broadcasted_iota(jnp.int32, (8, size), 1)
    sublane = lax.broadcasted_iota(jnp.int32, (8, size), 0)
    finished = []
    for g in range(size // 8):
        result = jnp.zeros((8, size), jnp.float32)
        for s in range(8):
            j = 8 * g + s
            row = jnp.broadcast_to(groups[g][s : s + 1, :], (8, size))
            pivot = jnp.broadcast_to(row[:, j : j + 1], (8, size))
            at_pivot = lane == j
            row = jnp.where(at_pivot, 1.0, row)
            scaled = row * (1.0 / pivot)
            result = jnp.where(
                (sublane == s) & (lane <= j), row * (1.0 / jnp.sqrt(pivot)), result
            )
            for i in range(g, size // 8):
                column = jnp.broadcast_to(groups[i][:, j : j + 1], (8, size))
                groups[i] = jnp.where(at_pivot, 0.0, groups[i]) - column * scaled if i > g else (
                    jnp.where(
                        sublane > s,
                        jnp.where(at_pivot, 0.0, groups[i]) - column * scaled,
                        groups[i],
                    )
                )
        finished.append(result)
    return jnp.concatenate(finished, axis=0)


def inverse_factor_kernel(size, block, margin_ref, out_ref, work, panel):
    work[...] = margin_ref[...]
    count = size // block

    @pl.loop(0, count)
    def _(k):
        here = pl.ds(pl.multiple_of(k * block, block), block)
        inverse = block_inverse_factor(work[here, here])
        rows = dot_in_kernel(inverse, work[here, :], ((1,), (0,)))
        panel[...] = rows
        work[here, :] = rows
        work[here, here] = inverse

        @pl.loop(k + 1, count)
        def _(i):
            there = pl.ds(pl.multiple_of(i * block, block), block)
            work[there, here] = jnp.zeros((block, block), jnp.float32)
            work[there, :] = work[there, :] - dot_in_kernel(
                panel[:, there], work[here, :], ((0,), (0,))
            )

    for r in range(count):
        rows = pl.ds(r * block, block)
        out_ref[rows, :] = jnp.zeros((block, size), jnp.float32)
        out_ref[rows, : (r + 1) * block] = work[rows, : (r + 1) * block]


def inverse_factor(margin, block):
    size = margin.shape[0]
    return pl.pallas_call(
        functools.partial(inverse_factor_kernel, size, block),
        out_shape=jax.ShapeDtypeStruct((size, size), jnp.float32),
        in_specs=[VMEM],
        out_specs=VMEM,
        scratch_shapes=[
            pltpu.VMEM((size, size), jnp.float32),
            pltpu.VMEM((block, size), jnp.float32),
        ],
    )(margin)


def greet(axis, count, me):
    barrier = pltpu.get_barrier_semaphore()
    for k in range(1, count):
        pl.semaphore_signal(
            barrier, inc=1, device_id={axis: lax.rem(me + k, count)}, device_id_type=MESH
        )
    pl.semaphore_wait(barrier, count - 1)


def remote(axis, peer, source, target, send_sem, recv_sem):
    return pltpu.make_async_remote_copy(
        src_ref=source,
        dst_ref=target,
        send_sem=send_sem,
        recv_sem=recv_sem,
        device_id={axis: peer},
        device_id_type=MESH,
    )


def grid_sum_kernel(count, x_ref, out_ref, parts, mine, total, s1, r1, s2, r2):
    me = lax.axis_index("grid")
    chunk = x_ref.shape[0] // count
    greet("grid", count, me)
    copies = []
    for k in range(1, count):
        peer = lax.rem(me + k, count)
        copy = remote(
            "grid",
            peer,
            x_ref.at[pl.ds(pl.multiple_of(peer * chunk, chunk), chunk), :],
            parts.at[k - 1],
            s1.at[k - 1],
            r1.at[k - 1],
        )
        copy.start()
        copies.append(copy)
    own = pl.ds(pl.multiple_of(me * chunk, chunk), chunk)
    mine[...] = x_ref[own, :]
    for k in range(1, count):
        copies[k - 1].wait_recv()
        mine[...] += parts[k - 1]
    total[me] = mine[...]
    back = []
    for k in range(1, count):
        peer = lax.rem(me + k, count)
        copy = remote("grid", peer, mine, total.at[me], s2.at[k - 1], r2.at[k - 1])
        copy.start()
        back.append(copy)
    for k in range(1, count):
        copies[k - 1].wait_send()
        back[k - 1].wait()
    for c in range(count):
        out_ref[c * chunk : (c + 1) * chunk, :] = total[c]


def grid_sum(x):
    count = lax.axis_size("grid")
    rows, columns = x.shape
    chunk = rows // count
    sems = pltpu.SemaphoreType.DMA((count - 1,))
    return pl.pallas_call(
        functools.partial(grid_sum_kernel, count),
        out_shape=jax.ShapeDtypeStruct(x.shape, jnp.float32),
        in_specs=[VMEM],
        out_specs=VMEM,
        scratch_shapes=[
            pltpu.VMEM((count - 1, chunk, columns), jnp.float32),
            pltpu.VMEM((chunk, columns), jnp.float32),
            pltpu.VMEM((count, chunk, columns), jnp.float32),
            sems,
            sems,
            sems,
            sems,
        ],
        compiler_params=pltpu.CompilerParams(collective_id=1, has_side_effects=True),
        cost_estimate=pl.CostEstimate(flops=10**6, bytes_accessed=4 * 10**7, transcendentals=0),
    )(x)


def band_gather_kernel(count, x_ref, out_ref, held, send, recv):
    me = lax.axis_index("band")
    width = x_ref.shape[1]
    if count == 4:
        half, side = lax.div(me, 2), lax.rem(me, 2)
        partner = half * 2 + 1 - side
        across = (1 - half) * 2 + side
        barrier = pltpu.get_barrier_semaphore()
        for peer in (partner, across):
            pl.semaphore_signal(barrier, inc=1, device_id={"band": peer}, device_id_type=MESH)
        pl.semaphore_wait(barrier, 2)
        far = remote("band", across, x_ref, held.at[0], send.at[0], recv.at[0])
        far.start()
        near = remote("band", partner, x_ref, held.at[1], send.at[1], recv.at[1])
        near.start()
        out_ref[:, pl.ds(pl.multiple_of(me * width, width), width)] = x_ref[...]
        far.wait_recv()
        relay = remote("band", partner, held.at[0], held.at[2], send.at[2], recv.at[2])
        relay.start()
        near.wait_recv()
        out_ref[:, pl.ds(pl.multiple_of(partner * width, width), width)] = held[1]
        out_ref[:, pl.ds(pl.multiple_of(across * width, width), width)] = held[0]
        relay.wait_recv()
        opposite = (1 - half) * 2 + 1 - side
        out_ref[:, pl.ds(pl.multiple_of(opposite * width, width), width)] = held[2]
        far.wait_send()
        near.wait_send()
        relay.wait_send()
    else:
        greet("band", count, me)
        copies = []
        for k in range(1, count):
            peer = lax.rem(me + k, count)
            copy = remote("band", peer, x_ref, held.at[k - 1], send.at[k - 1], recv.at[k - 1])
            copy.start()
            copies.append(copy)
        out_ref[:, pl.ds(pl.multiple_of(me * width, width), width)] = x_ref[...]
        for k in range(1, count):
            copies[k - 1].wait()
            source = lax.rem(me + count - k, count)
            out_ref[:, pl.ds(pl.multiple_of(source * width, width), width)] = held[k - 1]


def band_gather(x, collective):
    count = lax.axis_size("band")
    rows, columns = x.shape
    return pl.pallas_call(
        functools.partial(band_gather_kernel, count),
        out_shape=jax.ShapeDtypeStruct((rows, columns * count), jnp.float32),
        in_specs=[VMEM],
        out_specs=VMEM,
        scratch_shapes=[
            pltpu.VMEM((count - 1, rows, columns), jnp.float32),
            pltpu.SemaphoreType.DMA((count - 1,)),
            pltpu.SemaphoreType.DMA((count - 1,)),
        ],
        compiler_params=pltpu.CompilerParams(collective_id=collective, has_side_effects=True),
        cost_estimate=pl.CostEstimate(flops=10**6, bytes_accessed=4 * 10**7, transcendentals=0),
    )(x)


def update_kernel(
    count, v_ref, w_ref, out_ref, quotient_ref, norm_ref, part1, part2, all1, all2, s1, r1, s2, r2
):
    me = lax.axis_index("grid")
    cells, bands = v_ref.shape
    greet("grid", count, me)

    def exchange(value, part, everyone, send, recv):
        part[...] = value
        everyone[me] = value
        copies = []
        for k in range(1, count):
            peer = lax.rem(me + k, count)
            copy = remote("grid", peer, part, everyone.at[me], send.at[k - 1], recv.at[k - 1])
            copy.start()
            copies.append(copy)
        for copy in copies:
            copy.wait()
        total = everyone[0]
        for c in range(1, count):
            total = total + everyone[c]
        return jnp.sum(total, axis=0, keepdims=True)

    products = v_ref[...] * w_ref[...]
    quotient = exchange(
        jnp.sum(products.reshape(cells // 8, 8, bands), axis=0), part1, all1, s1, r1
    )
    quotient_ref[...] = quotient
    residual = w_ref[...] - quotient * v_ref[...]
    squared = exchange(
        jnp.sum((residual * residual).reshape(cells // 8, 8, bands), axis=0), part2, all2, s2, r2
    )
    norm_ref[...] = jnp.sqrt(squared)
    factor = STEP_LENGTH / jnp.sqrt(squared + NORM_EPS)
    out_ref[...] = v_ref[...] - (w_ref[...] - quotient * v_ref[...]) * factor


def update(vectors, applied):
    count = lax.axis_size("grid")
    bands = vectors.shape[1]
    sems = pltpu.SemaphoreType.DMA((count - 1,))
    small = pltpu.VMEM((8, bands), jnp.float32)
    everyone = pltpu.VMEM((count, 8, bands), jnp.float32)
    line = jax.ShapeDtypeStruct((1, bands), jnp.float32)
    return pl.pallas_call(
        functools.partial(update_kernel, count),
        out_shape=(jax.ShapeDtypeStruct(vectors.shape, jnp.float32), line, line),
        in_specs=[VMEM, VMEM],
        out_specs=(VMEM, VMEM, VMEM),
        scratch_shapes=[small, small, everyone, everyone, sems, sems, sems, sems],
        compiler_params=pltpu.CompilerParams(collective_id=4, has_side_effects=True),
    )(vectors, applied)


def local(orbitals, projectors, potential):
    grid_shape = orbitals.shape
    local_bands = orbitals.shape[3]
    first_band = lax.axis_index("band") * local_bands
    vectors = orbitals.reshape(-1, local_bands)
    every_projector = lax.all_gather(projectors, "band", axis=3, tiled=True).reshape(
        -1, projectors.shape[3] * lax.axis_size("band")
    )
    quotient_list = []
    norm_list = []
    for iteration in range(ITERS):
        gathered = band_gather(vectors, 2)
        margin = band_gather(grid_sum(matmul(gathered.T, vectors)), 3)
        inverse = inverse_factor(margin, local_bands)
        rows = lax.dynamic_slice_in_dim(inverse, first_band, local_bands, 0)
        vectors = lax.dot_general(
            gathered,
            rows,
            (((1,), (1,)), ((), ())),
            precision=HIGHEST,
            preferred_element_type=jnp.float32,
        )
        coupling = grid_sum(matmul(every_projector.T, vectors))
        exchange_part = matmul(every_projector, coupling)
        grid_field = vectors.reshape(grid_shape)
        applied = (-0.5 * laplacian(grid_field) + potential[..., None] * grid_field).reshape(
            -1, local_bands
        ) - exchange_part
        vectors, rayleigh, norm = update(vectors, applied)
        quotient_list.append(rayleigh)
        norm_list.append(norm)
    return (
        vectors.reshape(grid_shape),
        jnp.concatenate(quotient_list, axis=0),
        jnp.concatenate(norm_list, axis=0),
    )


def solution(mesh):
    return jax.shard_map(
        local,
        mesh=mesh,
        in_specs=(
            P("grid", None, None, "band"),
            P("grid", None, None, "band"),
            P("grid", None, None),
        ),
        out_specs=(P("grid", None, None, "band"), P(None, "band"), P(None, "band")),
        check_vma=False,
    )
```

```python
import functools

import jax
import jax.numpy as jnp
from jax import lax
from jax.experimental import pallas as pl
from jax.experimental.pallas import tpu as pltpu
from jax.sharding import PartitionSpec as P

ITERS = 3


STENCIL = (-205.0 / 72.0, 8.0 / 5.0, -1.0 / 5.0, 8.0 / 315.0, -1.0 / 560.0)
STEP_LENGTH = 0.25
NORM_EPS = 1e-06
HIGHEST = lax.Precision.HIGHEST
MESH = pl.DeviceIdType.MESH
VMEM = pl.BlockSpec(memory_space=pltpu.VMEM)


def matmul(left, right, precision=HIGHEST):
    return jnp.dot(left, right, precision=precision, preferred_element_type=jnp.float32)


def laplacian(grid_field, low, high):
    padded = jnp.concatenate([low, grid_field, high], axis=0)
    planes_here = grid_field.shape[0]
    result = 3.0 * STENCIL[0] * grid_field
    for distance in range(1, 5):
        result = result + STENCIL[distance] * (
            padded[4 + distance : 4 + distance + planes_here]
            + padded[4 - distance : 4 - distance + planes_here]
        )
    for dimension in (1, 2):
        for distance in range(1, 5):
            result = result + STENCIL[distance] * (
                jnp.roll(grid_field, distance, dimension)
                + jnp.roll(grid_field, -distance, dimension)
            )
    return result


def dot_in_kernel(left, right, contract):
    return lax.dot_general(
        left, right, (contract, ((), ())), precision=HIGHEST, preferred_element_type=jnp.float32
    )


def block_inverse_factor(block):
    size = block.shape[0]
    groups = [block[8 * g : 8 * g + 8, :] for g in range(size // 8)]
    lane = lax.broadcasted_iota(jnp.int32, (8, size), 1)
    sublane = lax.broadcasted_iota(jnp.int32, (8, size), 0)

    def spread_row(value, s):
        return jnp.broadcast_to(value[s : s + 1, :], (8, size))

    def spread_column(value, j):
        return jnp.broadcast_to(value[:, j : j + 1], (8, size))

    finished = []
    for g in range(size // 8):
        first = 8 * g
        inside = (lane >= first) & (lane < first + 8)
        columns = [spread_column(groups[g], first + t) for t in range(8)]
        entry = [[spread_row(columns[t], s) for t in range(s + 1)] for s in range(8)]
        start = jnp.where(inside, jnp.where(lane - first == sublane, 1.0, 0.0), groups[g])
        rows = [spread_row(start, s) for s in range(8)]
        inverse_pivot = []
        factor = [[None] * 8 for _ in range(8)]
        for t in range(8):
            inverse_pivot.append(1.0 / entry[t][t])
            for s in range(t + 1, 8):
                factor[s][t] = entry[s][t] * inverse_pivot[t]
                for u in range(t + 1, s + 1):
                    entry[s][u] = entry[s][u] - factor[s][t] * entry[u][t]
                rows[s] = rows[s] - factor[s][t] * rows[t]
        result = jnp.zeros((8, size), jnp.float32)
        for s in range(8):
            result = jnp.where(sublane == s, rows[s] * (1.0 / jnp.sqrt(entry[s][s])), result)
        finished.append(jnp.where(lane < first + 8, result, 0.0))
        solved = [None] * 8
        for s in reversed(range(8)):
            solved[s] = rows[s] * inverse_pivot[s]
            for t in range(s + 1, 8):
                solved[s] = solved[s] - factor[t][s] * solved[t]
        for i in range(g + 1, size // 8):
            value = jnp.where(inside, 0.0, groups[i])
            for t in range(8):
                value = value - spread_column(groups[i], first + t) * solved[t]
            groups[i] = value
    return jnp.concatenate(finished, axis=0)


def inverse_factor_kernel(size, block, margin_ref, out_ref, work, panel):
    work[...] = margin_ref[...]
    count = size // block

    @pl.loop(0, count)
    def _(k):
        here = pl.ds(pl.multiple_of(k * block, block), block)
        inverse = block_inverse_factor(work[here, here])
        rows = dot_in_kernel(inverse, work[here, :], ((1,), (0,)))
        panel[...] = rows
        work[here, :] = rows
        work[here, here] = inverse

        @pl.loop(k + 1, count)
        def _(i):
            there = pl.ds(pl.multiple_of(i * block, block), block)
            work[there, here] = jnp.zeros((block, block), jnp.float32)
            work[there, :] = work[there, :] - dot_in_kernel(
                panel[:, there], work[here, :], ((0,), (0,))
            )

    for r in range(count):
        rows = pl.ds(r * block, block)
        out_ref[rows, :] = jnp.zeros((block, size), jnp.float32)
        out_ref[rows, : (r + 1) * block] = work[rows, : (r + 1) * block]


def inverse_factor(margin, block):
    size = margin.shape[0]
    return pl.pallas_call(
        functools.partial(inverse_factor_kernel, size, block),
        out_shape=jax.ShapeDtypeStruct((size, size), jnp.float32),
        in_specs=[VMEM],
        out_specs=VMEM,
        scratch_shapes=[
            pltpu.VMEM((size, size), jnp.float32),
            pltpu.VMEM((block, size), jnp.float32),
        ],
    )(margin)


def greet(axis, count, me):
    barrier = pltpu.get_barrier_semaphore()
    for k in range(1, count):
        pl.semaphore_signal(
            barrier, inc=1, device_id={axis: lax.rem(me + k, count)}, device_id_type=MESH
        )
    pl.semaphore_wait(barrier, count - 1)


def remote(axis, peer, source, target, send_sem, recv_sem):
    return pltpu.make_async_remote_copy(
        src_ref=source,
        dst_ref=target,
        send_sem=send_sem,
        recv_sem=recv_sem,
        device_id={axis: peer},
        device_id_type=MESH,
    )


def ring_places(count):
    me = lax.axis_index("band")
    half, side = lax.div(me, 2), lax.rem(me, 2)
    partner = half * 2 + 1 - side
    across = (1 - half) * 2 + side
    return me, partner, across, (1 - half) * 2 + 1 - side


def grid_sum_kernel(count, bands, edge, kind, *refs):
    refs = list(refs)
    x_ref = refs.pop(0)
    extra = refs.pop(0) if kind else None
    out_ref = refs.pop(0)
    extra_out = [refs.pop(0) for _ in range({"": 0, "gather": 1, "halo": 2}[kind])]
    parts, mine, total, s1, r1, s2, r2 = refs[:7]
    me = lax.axis_index("grid")
    chunk = x_ref.shape[0] // count
    barrier = pltpu.get_barrier_semaphore()
    for k in range(1, count):
        pl.semaphore_signal(
            barrier, inc=1, device_id={"grid": lax.rem(me + k, count)}, device_id_type=MESH
        )
    greeted = count - 1
    if kind == "gather":
        place, partner, across, opposite = ring_places(bands)
        for peer in (partner, across):
            pl.semaphore_signal(barrier, inc=1, device_id={"band": peer}, device_id_type=MESH)
        greeted += 2
    pl.semaphore_wait(barrier, greeted)
    if kind == "gather":
        held, send, recv = refs[7:]
        far = remote("band", across, extra, held.at[0], send.at[0], recv.at[0])
        near = remote("band", partner, extra, held.at[1], send.at[1], recv.at[1])
        far.start()
        near.start()
    copies = []
    for k in range(1, count):
        peer = lax.rem(me + k, count)
        copy = remote(
            "grid",
            peer,
            x_ref.at[pl.ds(pl.multiple_of(peer * chunk, chunk), chunk), :],
            parts.at[k - 1],
            s1.at[k - 1],
            r1.at[k - 1],
        )
        copy.start()
        copies.append(copy)
    if kind == "halo":
        held, send, recv = refs[7:]
        cells = extra.shape[0]
        after = remote(
            "grid",
            lax.rem(me + 1, count),
            extra.at[pl.ds(cells - edge, edge), :],
            held.at[0],
            send.at[0],
            recv.at[0],
        )
        before = remote(
            "grid",
            lax.rem(me + count - 1, count),
            extra.at[pl.ds(0, edge), :],
            held.at[1],
            send.at[1],
            recv.at[1],
        )
    own = pl.ds(pl.multiple_of(me * chunk, chunk), chunk)
    mine[...] = x_ref[own, :]
    for k in range(1, count):
        copies[k - 1].wait_recv()
        mine[...] += parts[k - 1]
    total[me] = mine[...]
    back = []
    for k in range(1, count):
        peer = lax.rem(me + k, count)
        copy = remote("grid", peer, mine, total.at[me], s2.at[k - 1], r2.at[k - 1])
        copy.start()
        back.append(copy)
    if kind == "halo":
        after.start()
        before.start()
    if kind == "gather":
        width = extra.shape[1]

        def put(source, value):
            extra_out[0][:, pl.ds(pl.multiple_of(source * width, width), width)] = value

        far.wait_recv()
        relay = remote("band", partner, held.at[0], held.at[2], send.at[2], recv.at[2])
        relay.start()
        put(place, extra[...])
        near.wait_recv()
        put(partner, held[1])
        put(across, held[0])
        relay.wait_recv()
        put(opposite, held[2])
        far.wait_send()
        near.wait_send()
        relay.wait_send()
    for k in range(1, count):
        copies[k - 1].wait_send()
        back[k - 1].wait()
    for c in range(count):
        out_ref[c * chunk : (c + 1) * chunk, :] = total[c]
    if kind == "halo":
        after.wait()
        before.wait()
        extra_out[0][...] = held[0]
        extra_out[1][...] = held[1]


def grid_sum(x, collective, kind="", extra=None, edge=0):
    count = lax.axis_size("grid")
    bands = lax.axis_size("band")
    rows, columns = x.shape
    chunk = rows // count
    sems = pltpu.SemaphoreType.DMA((count - 1,))
    out_shape = [jax.ShapeDtypeStruct(x.shape, jnp.float32)]
    more = []
    if kind == "gather":
        cells, width = extra.shape
        out_shape.append(jax.ShapeDtypeStruct((cells, width * bands), jnp.float32))
        more = [pltpu.VMEM((3, cells, width), jnp.float32)]
        more += [pltpu.SemaphoreType.DMA((3,))] * 2
    if kind == "halo":
        width = extra.shape[1]
        out_shape += [jax.ShapeDtypeStruct((edge, width), jnp.float32)] * 2
        more = [pltpu.VMEM((2, edge, width), jnp.float32)]
        more += [pltpu.SemaphoreType.DMA((2,))] * 2
    operands = [x] + ([extra] if kind else [])
    result = pl.pallas_call(
        functools.partial(grid_sum_kernel, count, bands, edge, kind),
        out_shape=out_shape,
        in_specs=[VMEM] * len(operands),
        out_specs=[VMEM] * len(out_shape),
        scratch_shapes=[
            pltpu.VMEM((count - 1, chunk, columns), jnp.float32),
            pltpu.VMEM((chunk, columns), jnp.float32),
            pltpu.VMEM((count, chunk, columns), jnp.float32),
            sems,
            sems,
            sems,
            sems,
        ]
        + more,
        compiler_params=pltpu.CompilerParams(collective_id=collective, has_side_effects=True),
        cost_estimate=pl.CostEstimate(flops=10**6, bytes_accessed=4 * 10**7, transcendentals=0),
    )(*operands)
    return result


def band_gather_kernel(count, x_ref, out_ref, held, send, recv):
    me = lax.axis_index("band")
    width = x_ref.shape[1]
    if count == 4:
        half, side = lax.div(me, 2), lax.rem(me, 2)
        partner = half * 2 + 1 - side
        across = (1 - half) * 2 + side
        barrier = pltpu.get_barrier_semaphore()
        for peer in (partner, across):
            pl.semaphore_signal(barrier, inc=1, device_id={"band": peer}, device_id_type=MESH)
        pl.semaphore_wait(barrier, 2)
        far = remote("band", across, x_ref, held.at[0], send.at[0], recv.at[0])
        far.start()
        near = remote("band", partner, x_ref, held.at[1], send.at[1], recv.at[1])
        near.start()
        out_ref[:, pl.ds(pl.multiple_of(me * width, width), width)] = x_ref[...]
        far.wait_recv()
        relay = remote("band", partner, held.at[0], held.at[2], send.at[2], recv.at[2])
        relay.start()
        near.wait_recv()
        out_ref[:, pl.ds(pl.multiple_of(partner * width, width), width)] = held[1]
        out_ref[:, pl.ds(pl.multiple_of(across * width, width), width)] = held[0]
        relay.wait_recv()
        opposite = (1 - half) * 2 + 1 - side
        out_ref[:, pl.ds(pl.multiple_of(opposite * width, width), width)] = held[2]
        far.wait_send()
        near.wait_send()
        relay.wait_send()
    else:
        greet("band", count, me)
        copies = []
        for k in range(1, count):
            peer = lax.rem(me + k, count)
            copy = remote("band", peer, x_ref, held.at[k - 1], send.at[k - 1], recv.at[k - 1])
            copy.start()
            copies.append(copy)
        out_ref[:, pl.ds(pl.multiple_of(me * width, width), width)] = x_ref[...]
        for k in range(1, count):
            copies[k - 1].wait()
            source = lax.rem(me + count - k, count)
            out_ref[:, pl.ds(pl.multiple_of(source * width, width), width)] = held[k - 1]


def band_gather(x, collective):
    count = lax.axis_size("band")
    rows, columns = x.shape
    return pl.pallas_call(
        functools.partial(band_gather_kernel, count),
        out_shape=jax.ShapeDtypeStruct((rows, columns * count), jnp.float32),
        in_specs=[VMEM],
        out_specs=VMEM,
        scratch_shapes=[
            pltpu.VMEM((count - 1, rows, columns), jnp.float32),
            pltpu.SemaphoreType.DMA((count - 1,)),
            pltpu.SemaphoreType.DMA((count - 1,)),
        ],
        compiler_params=pltpu.CompilerParams(collective_id=collective, has_side_effects=True),
        cost_estimate=pl.CostEstimate(flops=10**6, bytes_accessed=4 * 10**7, transcendentals=0),
    )(x)


def update_kernel(
    count, v_ref, w_ref, out_ref, quotient_ref, norm_ref, part1, part2, all1, all2, s1, r1, s2, r2
):
    me = lax.axis_index("grid")
    cells, bands = v_ref.shape
    greet("grid", count, me)

    def exchange(value, part, everyone, send, recv):
        part[...] = value
        everyone[me] = value
        copies = []
        for k in range(1, count):
            peer = lax.rem(me + k, count)
            copy = remote("grid", peer, part, everyone.at[me], send.at[k - 1], recv.at[k - 1])
            copy.start()
            copies.append(copy)
        for copy in copies:
            copy.wait()
        total = everyone[0]
        for c in range(1, count):
            total = total + everyone[c]
        return jnp.sum(total, axis=0, keepdims=True)

    products = v_ref[...] * w_ref[...]
    quotient = exchange(
        jnp.sum(products.reshape(cells // 8, 8, bands), axis=0), part1, all1, s1, r1
    )
    quotient_ref[...] = quotient
    residual = w_ref[...] - quotient * v_ref[...]
    squared = exchange(
        jnp.sum((residual * residual).reshape(cells // 8, 8, bands), axis=0), part2, all2, s2, r2
    )
    norm_ref[...] = jnp.sqrt(squared)
    factor = STEP_LENGTH / jnp.sqrt(squared + NORM_EPS)
    out_ref[...] = v_ref[...] - (w_ref[...] - quotient * v_ref[...]) * factor


def update(vectors, applied):
    count = lax.axis_size("grid")
    bands = vectors.shape[1]
    sems = pltpu.SemaphoreType.DMA((count - 1,))
    small = pltpu.VMEM((8, bands), jnp.float32)
    everyone = pltpu.VMEM((count, 8, bands), jnp.float32)
    line = jax.ShapeDtypeStruct((1, bands), jnp.float32)
    return pl.pallas_call(
        functools.partial(update_kernel, count),
        out_shape=(jax.ShapeDtypeStruct(vectors.shape, jnp.float32), line, line),
        in_specs=[VMEM, VMEM],
        out_specs=(VMEM, VMEM, VMEM),
        scratch_shapes=[small, small, everyone, everyone, sems, sems, sems, sems],
        compiler_params=pltpu.CompilerParams(collective_id=4, has_side_effects=True),
    )(vectors, applied)


def local(orbitals, projectors, potential):
    grid_shape = orbitals.shape
    local_bands = orbitals.shape[3]
    first_band = lax.axis_index("band") * local_bands
    vectors = orbitals.reshape(-1, local_bands)
    plane = vectors.shape[0] // grid_shape[0]
    projector_rows = projectors.reshape(-1, projectors.shape[3])
    joined = lax.axis_size("band") == 4
    if not joined:
        every_projector = band_gather(projector_rows, 3)
    quotient_list = []
    norm_list = []
    for iteration in range(ITERS):
        gathered = band_gather(vectors, 2)
        share = matmul(gathered.T, vectors)
        if iteration == 0 and joined:
            summed, every_projector = grid_sum(share, 5, "gather", projector_rows)
        else:
            (summed,) = grid_sum(share, 1)
        margin = band_gather(summed, 6)
        inverse = inverse_factor(margin, local_bands)
        rows = lax.dynamic_slice_in_dim(inverse, first_band, local_bands, 0)
        vectors = lax.dot_general(
            gathered,
            rows,
            (((1,), (1,)), ((), ())),
            precision=HIGHEST,
            preferred_element_type=jnp.float32,
        )
        coupling, low, high = grid_sum(
            matmul(every_projector.T, vectors, lax.Precision.HIGH), 7, "halo", vectors, 4 * plane
        )
        exchange_part = matmul(every_projector, coupling, lax.Precision.HIGH)
        grid_field = vectors.reshape(grid_shape)
        applied = (-0.5 * laplacian(
            grid_field, low.reshape(4, *grid_shape[1:]), high.reshape(4, *grid_shape[1:])
        ) + potential[..., None] * grid_field).reshape(
            -1, local_bands
        ) - exchange_part
        vectors, rayleigh, norm = update(vectors, applied)
        quotient_list.append(rayleigh)
        norm_list.append(norm)
    return (
        vectors.reshape(grid_shape),
        jnp.concatenate(quotient_list, axis=0),
        jnp.concatenate(norm_list, axis=0),
    )


def solution(mesh):
    return jax.shard_map(
        local,
        mesh=mesh,
        in_specs=(
            P("grid", None, None, "band"),
            P("grid", None, None, "band"),
            P("grid", None, None),
        ),
        out_specs=(P("grid", None, None, "band"), P(None, "band"), P(None, "band")),
        check_vma=False,
    )
```

```python
import functools

import jax
import jax.numpy as jnp
from jax import lax
from jax.experimental import pallas as pl
from jax.experimental.pallas import tpu as pltpu
from jax.sharding import PartitionSpec as P

ITERS = 3


STENCIL = (-205.0 / 72.0, 8.0 / 5.0, -1.0 / 5.0, 8.0 / 315.0, -1.0 / 560.0)
STEP_LENGTH = 0.25
NORM_EPS = 1e-06
HIGHEST = lax.Precision.HIGHEST
MESH = pl.DeviceIdType.MESH
VMEM = pl.BlockSpec(memory_space=pltpu.VMEM)


def matmul(left, right, precision=HIGHEST):
    return jnp.dot(left, right, precision=precision, preferred_element_type=jnp.float32)


def laplacian(grid_field, low, high):
    padded = jnp.concatenate([low, grid_field, high], axis=0)
    planes_here = grid_field.shape[0]
    result = 3.0 * STENCIL[0] * grid_field
    for distance in range(1, 5):
        result = result + STENCIL[distance] * (
            padded[4 + distance : 4 + distance + planes_here]
            + padded[4 - distance : 4 - distance + planes_here]
        )
    for dimension in (1, 2):
        for distance in range(1, 5):
            result = result + STENCIL[distance] * (
                jnp.roll(grid_field, distance, dimension)
                + jnp.roll(grid_field, -distance, dimension)
            )
    return result


def dot_in_kernel(left, right, contract):
    return lax.dot_general(
        left, right, (contract, ((), ())), precision=HIGHEST, preferred_element_type=jnp.float32
    )


def block_inverse_factor(block):
    size = block.shape[0]
    groups = [block[8 * g : 8 * g + 8, :] for g in range(size // 8)]
    lane = lax.broadcasted_iota(jnp.int32, (8, size), 1)
    sublane = lax.broadcasted_iota(jnp.int32, (8, size), 0)

    def spread_row(value, s):
        return jnp.broadcast_to(value[s : s + 1, :], (8, size))

    def spread_column(value, j):
        return jnp.broadcast_to(value[:, j : j + 1], (8, size))

    finished = []
    for g in range(size // 8):
        first = 8 * g
        inside = (lane >= first) & (lane < first + 8)
        columns = [spread_column(groups[g], first + t) for t in range(8)]
        entry = [[spread_row(columns[t], s) for t in range(s + 1)] for s in range(8)]
        start = jnp.where(inside, jnp.where(lane - first == sublane, 1.0, 0.0), groups[g])
        rows = [spread_row(start, s) for s in range(8)]
        inverse_pivot = []
        factor = [[None] * 8 for _ in range(8)]
        for t in range(8):
            inverse_pivot.append(1.0 / entry[t][t])
            for s in range(t + 1, 8):
                factor[s][t] = entry[s][t] * inverse_pivot[t]
                for u in range(t + 1, s + 1):
                    entry[s][u] = entry[s][u] - factor[s][t] * entry[u][t]
                rows[s] = rows[s] - factor[s][t] * rows[t]
        result = jnp.zeros((8, size), jnp.float32)
        for s in range(8):
            result = jnp.where(sublane == s, rows[s] * (1.0 / jnp.sqrt(entry[s][s])), result)
        finished.append(jnp.where(lane < first + 8, result, 0.0))
        solved = [None] * 8
        for s in reversed(range(8)):
            solved[s] = rows[s] * inverse_pivot[s]
            for t in range(s + 1, 8):
                solved[s] = solved[s] - factor[t][s] * solved[t]
        for i in range(g + 1, size // 8):
            value = jnp.where(inside, 0.0, groups[i])
            for t in range(8):
                value = value - spread_column(groups[i], first + t) * solved[t]
            groups[i] = value
    return jnp.concatenate(finished, axis=0)


def inverse_factor_kernel(size, block, margin_ref, out_ref, work, panel):
    work[...] = margin_ref[...]
    count = size // block

    @pl.loop(0, count)
    def _(k):
        here = pl.ds(pl.multiple_of(k * block, block), block)
        inverse = block_inverse_factor(work[here, here])
        rows = dot_in_kernel(inverse, work[here, :], ((1,), (0,)))
        panel[...] = rows
        work[here, :] = rows
        work[here, here] = inverse

        @pl.loop(k + 1, count)
        def _(i):
            there = pl.ds(pl.multiple_of(i * block, block), block)
            work[there, here] = jnp.zeros((block, block), jnp.float32)
            work[there, :] = work[there, :] - dot_in_kernel(
                panel[:, there], work[here, :], ((0,), (0,))
            )

    for r in range(count):
        rows = pl.ds(r * block, block)
        out_ref[rows, :] = jnp.zeros((block, size), jnp.float32)
        out_ref[rows, : (r + 1) * block] = work[rows, : (r + 1) * block]


def inverse_factor(margin, block):
    size = margin.shape[0]
    return pl.pallas_call(
        functools.partial(inverse_factor_kernel, size, block),
        out_shape=jax.ShapeDtypeStruct((size, size), jnp.float32),
        in_specs=[VMEM],
        out_specs=VMEM,
        scratch_shapes=[
            pltpu.VMEM((size, size), jnp.float32),
            pltpu.VMEM((block, size), jnp.float32),
        ],
    )(margin)


def greet(axis, count, me):
    barrier = pltpu.get_barrier_semaphore()
    for k in range(1, count):
        pl.semaphore_signal(
            barrier, inc=1, device_id={axis: lax.rem(me + k, count)}, device_id_type=MESH
        )
    pl.semaphore_wait(barrier, count - 1)


def remote(axis, peer, source, target, send_sem, recv_sem):
    return pltpu.make_async_remote_copy(
        src_ref=source,
        dst_ref=target,
        send_sem=send_sem,
        recv_sem=recv_sem,
        device_id={axis: peer},
        device_id_type=MESH,
    )


def ring_places(count):
    me = lax.axis_index("band")
    half, side = lax.div(me, 2), lax.rem(me, 2)
    partner = half * 2 + 1 - side
    across = (1 - half) * 2 + side
    return me, partner, across, (1 - half) * 2 + 1 - side


def grid_sum_kernel(count, bands, edge, kind, *refs):
    refs = list(refs)
    x_ref = refs.pop(0)
    extra = refs.pop(0) if kind else None
    out_ref = refs.pop(0)
    extra_out = [refs.pop(0) for _ in range({"": 0, "gather": 1, "halo": 2}[kind])]
    parts, mine, total, s1, r1, s2, r2 = refs[:7]
    me = lax.axis_index("grid")
    chunk = x_ref.shape[0] // count
    barrier = pltpu.get_barrier_semaphore()
    for k in range(1, count):
        pl.semaphore_signal(
            barrier, inc=1, device_id={"grid": lax.rem(me + k, count)}, device_id_type=MESH
        )
    greeted = count - 1
    if kind == "gather":
        place, partner, across, opposite = ring_places(bands)
        for peer in (partner, across):
            pl.semaphore_signal(barrier, inc=1, device_id={"band": peer}, device_id_type=MESH)
        greeted += 2
    pl.semaphore_wait(barrier, greeted)
    if kind == "gather":
        held, send, recv = refs[7:]
        far = remote("band", across, extra, held.at[0], send.at[0], recv.at[0])
        near = remote("band", partner, extra, held.at[1], send.at[1], recv.at[1])
        far.start()
        near.start()
    copies = []
    for k in range(1, count):
        peer = lax.rem(me + k, count)
        copy = remote(
            "grid",
            peer,
            x_ref.at[pl.ds(pl.multiple_of(peer * chunk, chunk), chunk), :],
            parts.at[k - 1],
            s1.at[k - 1],
            r1.at[k - 1],
        )
        copy.start()
        copies.append(copy)
    if kind == "halo":
        held, send, recv = refs[7:]
        cells = extra.shape[0]
        after = remote(
            "grid",
            lax.rem(me + 1, count),
            extra.at[pl.ds(cells - edge, edge), :],
            held.at[0],
            send.at[0],
            recv.at[0],
        )
        before = remote(
            "grid",
            lax.rem(me + count - 1, count),
            extra.at[pl.ds(0, edge), :],
            held.at[1],
            send.at[1],
            recv.at[1],
        )
        after.start()
        before.start()
    own = pl.ds(pl.multiple_of(me * chunk, chunk), chunk)
    mine[...] = x_ref[own, :]
    for k in range(1, count):
        copies[k - 1].wait_recv()
        mine[...] += parts[k - 1]
    total[me] = mine[...]
    back = []
    for k in range(1, count):
        peer = lax.rem(me + k, count)
        copy = remote("grid", peer, mine, total.at[me], s2.at[k - 1], r2.at[k - 1])
        copy.start()
        back.append(copy)
    if kind == "gather":
        width = extra.shape[1]

        def put(source, value):
            extra_out[0][:, pl.ds(pl.multiple_of(source * width, width), width)] = value

        far.wait_recv()
        relay = remote("band", partner, held.at[0], held.at[2], send.at[2], recv.at[2])
        relay.start()
        put(place, extra[...])
        near.wait_recv()
        put(partner, held[1])
        put(across, held[0])
        relay.wait_recv()
        put(opposite, held[2])
        far.wait_send()
        near.wait_send()
        relay.wait_send()
    for k in range(1, count):
        copies[k - 1].wait_send()
        back[k - 1].wait()
    for c in range(count):
        out_ref[c * chunk : (c + 1) * chunk, :] = total[c]
    if kind == "halo":
        after.wait()
        before.wait()
        extra_out[0][...] = held[0]
        extra_out[1][...] = held[1]


def grid_sum(x, collective, kind="", extra=None, edge=0):
    count = lax.axis_size("grid")
    bands = lax.axis_size("band")
    rows, columns = x.shape
    chunk = rows // count
    sems = pltpu.SemaphoreType.DMA((count - 1,))
    out_shape = [jax.ShapeDtypeStruct(x.shape, jnp.float32)]
    more = []
    if kind == "gather":
        cells, width = extra.shape
        out_shape.append(jax.ShapeDtypeStruct((cells, width * bands), jnp.float32))
        more = [pltpu.VMEM((3, cells, width), jnp.float32)]
        more += [pltpu.SemaphoreType.DMA((3,))] * 2
    if kind == "halo":
        width = extra.shape[1]
        out_shape += [jax.ShapeDtypeStruct((edge, width), jnp.float32)] * 2
        more = [pltpu.VMEM((2, edge, width), jnp.float32)]
        more += [pltpu.SemaphoreType.DMA((2,))] * 2
    operands = [x] + ([extra] if kind else [])
    result = pl.pallas_call(
        functools.partial(grid_sum_kernel, count, bands, edge, kind),
        out_shape=out_shape,
        in_specs=[VMEM] * len(operands),
        out_specs=[VMEM] * len(out_shape),
        scratch_shapes=[
            pltpu.VMEM((count - 1, chunk, columns), jnp.float32),
            pltpu.VMEM((chunk, columns), jnp.float32),
            pltpu.VMEM((count, chunk, columns), jnp.float32),
            sems,
            sems,
            sems,
            sems,
        ]
        + more,
        compiler_params=pltpu.CompilerParams(collective_id=collective, has_side_effects=True),
        cost_estimate=pl.CostEstimate(flops=10**6, bytes_accessed=4 * 10**7, transcendentals=0),
    )(*operands)
    return result


def band_gather_kernel(count, x_ref, out_ref, held, send, recv):
    me = lax.axis_index("band")
    width = x_ref.shape[1]
    if count == 4:
        half, side = lax.div(me, 2), lax.rem(me, 2)
        partner = half * 2 + 1 - side
        across = (1 - half) * 2 + side
        barrier = pltpu.get_barrier_semaphore()
        for peer in (partner, across):
            pl.semaphore_signal(barrier, inc=1, device_id={"band": peer}, device_id_type=MESH)
        pl.semaphore_wait(barrier, 2)
        far = remote("band", across, x_ref, held.at[0], send.at[0], recv.at[0])
        far.start()
        near = remote("band", partner, x_ref, held.at[1], send.at[1], recv.at[1])
        near.start()
        out_ref[:, pl.ds(pl.multiple_of(me * width, width), width)] = x_ref[...]
        far.wait_recv()
        relay = remote("band", partner, held.at[0], held.at[2], send.at[2], recv.at[2])
        relay.start()
        near.wait_recv()
        out_ref[:, pl.ds(pl.multiple_of(partner * width, width), width)] = held[1]
        out_ref[:, pl.ds(pl.multiple_of(across * width, width), width)] = held[0]
        relay.wait_recv()
        opposite = (1 - half) * 2 + 1 - side
        out_ref[:, pl.ds(pl.multiple_of(opposite * width, width), width)] = held[2]
        far.wait_send()
        near.wait_send()
        relay.wait_send()
    else:
        greet("band", count, me)
        copies = []
        for k in range(1, count):
            peer = lax.rem(me + k, count)
            copy = remote("band", peer, x_ref, held.at[k - 1], send.at[k - 1], recv.at[k - 1])
            copy.start()
            copies.append(copy)
        out_ref[:, pl.ds(pl.multiple_of(me * width, width), width)] = x_ref[...]
        for k in range(1, count):
            copies[k - 1].wait()
            source = lax.rem(me + count - k, count)
            out_ref[:, pl.ds(pl.multiple_of(source * width, width), width)] = held[k - 1]


def band_gather(x, collective):
    count = lax.axis_size("band")
    rows, columns = x.shape
    return pl.pallas_call(
        functools.partial(band_gather_kernel, count),
        out_shape=jax.ShapeDtypeStruct((rows, columns * count), jnp.float32),
        in_specs=[VMEM],
        out_specs=VMEM,
        scratch_shapes=[
            pltpu.VMEM((count - 1, rows, columns), jnp.float32),
            pltpu.SemaphoreType.DMA((count - 1,)),
            pltpu.SemaphoreType.DMA((count - 1,)),
        ],
        compiler_params=pltpu.CompilerParams(collective_id=collective, has_side_effects=True),
        cost_estimate=pl.CostEstimate(flops=10**6, bytes_accessed=4 * 10**7, transcendentals=0),
    )(x)


def update_kernel(
    count, v_ref, w_ref, out_ref, quotient_ref, norm_ref, part1, part2, all1, all2, s1, r1, s2, r2
):
    me = lax.axis_index("grid")
    cells, bands = v_ref.shape
    greet("grid", count, me)

    def exchange(value, part, everyone, send, recv):
        part[...] = value
        everyone[me] = value
        copies = []
        for k in range(1, count):
            peer = lax.rem(me + k, count)
            copy = remote("grid", peer, part, everyone.at[me], send.at[k - 1], recv.at[k - 1])
            copy.start()
            copies.append(copy)
        for copy in copies:
            copy.wait()
        total = everyone[0]
        for c in range(1, count):
            total = total + everyone[c]
        return jnp.sum(total, axis=0, keepdims=True)

    products = v_ref[...] * w_ref[...]
    quotient = exchange(
        jnp.sum(products.reshape(cells // 8, 8, bands), axis=0), part1, all1, s1, r1
    )
    quotient_ref[...] = quotient
    residual = w_ref[...] - quotient * v_ref[...]
    squared = exchange(
        jnp.sum((residual * residual).reshape(cells // 8, 8, bands), axis=0), part2, all2, s2, r2
    )
    norm_ref[...] = jnp.sqrt(squared)
    factor = STEP_LENGTH / jnp.sqrt(squared + NORM_EPS)
    out_ref[...] = v_ref[...] - (w_ref[...] - quotient * v_ref[...]) * factor


def update(vectors, applied):
    count = lax.axis_size("grid")
    bands = vectors.shape[1]
    sems = pltpu.SemaphoreType.DMA((count - 1,))
    small = pltpu.VMEM((8, bands), jnp.float32)
    everyone = pltpu.VMEM((count, 8, bands), jnp.float32)
    line = jax.ShapeDtypeStruct((1, bands), jnp.float32)
    return pl.pallas_call(
        functools.partial(update_kernel, count),
        out_shape=(jax.ShapeDtypeStruct(vectors.shape, jnp.float32), line, line),
        in_specs=[VMEM, VMEM],
        out_specs=(VMEM, VMEM, VMEM),
        scratch_shapes=[small, small, everyone, everyone, sems, sems, sems, sems],
        compiler_params=pltpu.CompilerParams(collective_id=4, has_side_effects=True),
    )(vectors, applied)


def local(orbitals, projectors, potential):
    grid_shape = orbitals.shape
    local_bands = orbitals.shape[3]
    first_band = lax.axis_index("band") * local_bands
    vectors = orbitals.reshape(-1, local_bands)
    plane = vectors.shape[0] // grid_shape[0]
    projector_rows = projectors.reshape(-1, projectors.shape[3])
    joined = lax.axis_size("band") == 4
    if not joined:
        every_projector = band_gather(projector_rows, 3)
    quotient_list = []
    norm_list = []
    for iteration in range(ITERS):
        gathered = band_gather(vectors, 2)
        share = matmul(gathered.T, vectors)
        if iteration == 0 and joined:
            summed, every_projector = grid_sum(share, 5, "gather", projector_rows)
        else:
            (summed,) = grid_sum(share, 1)
        margin = band_gather(summed, 6)
        inverse = inverse_factor(margin, local_bands)
        rows = lax.dynamic_slice_in_dim(inverse, first_band, local_bands, 0)
        vectors = lax.dot_general(
            gathered,
            rows,
            (((1,), (1,)), ((), ())),
            precision=HIGHEST,
            preferred_element_type=jnp.float32,
        )
        coupling, low, high = grid_sum(
            matmul(every_projector.T, vectors, lax.Precision.HIGH), 7, "halo", vectors, 4 * plane
        )
        exchange_part = matmul(every_projector, coupling, lax.Precision.HIGH)
        grid_field = vectors.reshape(grid_shape)
        applied = (-0.5 * laplacian(
            grid_field, low.reshape(4, *grid_shape[1:]), high.reshape(4, *grid_shape[1:])
        ) + potential[..., None] * grid_field).reshape(
            -1, local_bands
        ) - exchange_part
        vectors, rayleigh, norm = update(vectors, applied)
        quotient_list.append(rayleigh)
        norm_list.append(norm)
    return (
        vectors.reshape(grid_shape),
        jnp.concatenate(quotient_list, axis=0),
        jnp.concatenate(norm_list, axis=0),
    )


def solution(mesh):
    return jax.shard_map(
        local,
        mesh=mesh,
        in_specs=(
            P("grid", None, None, "band"),
            P("grid", None, None, "band"),
            P("grid", None, None),
        ),
        out_specs=(P("grid", None, None, "band"), P(None, "band"), P(None, "band")),
        check_vma=False,
    )
```
